32 devices in a mesh: row: 4 (over y, x), col: 8 (over z, core).
Axes of the slice: x: 2, y: 2, z: 4, core: 2. Of those that a mesh axis runs over, the one named last changes fastest.
Arguments:
- diag_inverse: bfloat16 [1376, 1376], P('row'), may hold values from -0.5 to 0.5, as said below
- row_u: bfloat16 [4, 1376, 224], P('row', None, 'col'), may hold values from -6 to 6
- row_v: bfloat16 [4, 1376, 224], P('row', None, 'col'), may hold values from -0.59765625 to 0.59765625
- col_u: bfloat16 [8, 1376, 224], P('col', None, 'row'), may hold values from -6 to 6
- col_v: bfloat16 [8, 1376, 224], P('col', None, 'row'), may hold values from -0.59765625 to 0.59765625
- tile_u: bfloat16 [4, 8, 1376, 224], P('row', 'col'), may hold values from -6 to 6
- tile_v: bfloat16 [4, 8, 1376, 224], P('row', 'col'), may hold values from -6 to 6
- sketch: bfloat16 [1376, 224], replicated, may hold values from -6 to 6
- row_rank: int32 [4], P('row'), may hold values from 56 to 224, as said below
- col_rank: int32 [8], P('col'), may hold values from 56 to 224, as said below
- old_rank: int32 [4, 8], P('row', 'col'), may hold values from 56 to 224, as said below
- new_rank: int32 [4, 8], P('row', 'col'), may hold values from 14 to 112, as said below
Outputs:
- new_u: bfloat16 [4, 8, 1376, 224], P('row', 'col')
- new_v: bfloat16 [4, 8, 1376, 224], P('row', 'col')
The draws below stay inside these ranges and needn't reach their ends.
Inputs may be any that keep to these rules, and one draw needn't show every extreme that they name: diag_inverse is lower triangular with diagonal entries between 0.25 and 0.5. `row_rank`: some tile has rank 224. `col_rank`: some tile has rank 224. `old_rank`: some tile has rank 224. `new_rank`: each entry lies between old_rank // 4 and old_rank // 2 of the same tile; some tile has rank 224 // 2.
All inputs are finite; a program needn't handle non-finite values.
Results may differ from the reference program's by a relative error of at most 0.0085.
Values may be sent and summed in bfloat16 or wider, within the bound.
No kernel may reach another device: no remote copies, remote signals or barrier semaphores. Data moves between devices by JAX's collectives and lax.ppermute only.
A program may use at most 64 MiB of HBM per device.

```python
import jax
import jax.numpy as jnp
from jax import lax

NB = 1376
RMAX = 224
TILE_ROWS = 4
TILE_COLS = 8


def panel_ranks(key, salt, count):
    folded = jax.random.fold_in(key, salt)
    key_rank, key_spot = jax.random.split(folded)
    ranks = jax.random.randint(key_rank, (count,), RMAX // 4, RMAX + 1, dtype=jnp.int32)
    forced = jax.random.randint(key_spot, (), 0, count, dtype=jnp.int32)
    return jnp.where(jnp.arange(count, dtype=jnp.int32) == forced, RMAX, ranks).astype(jnp.int32)


def rank_pair(key):
    folded = jax.random.fold_in(key, 11)
    key_old, key_spot, key_new = jax.random.split(folded, 3)
    cells = TILE_ROWS * TILE_COLS
    old_ranks = jax.random.randint(key_old, (cells,), RMAX // 4, RMAX + 1, dtype=jnp.int32)
    forced_cell = jax.random.randint(key_spot, (), 0, cells, dtype=jnp.int32)
    old_ranks = jnp.where(jnp.arange(cells, dtype=jnp.int32) == forced_cell, RMAX, old_ranks)
    lower_end = old_ranks // 4
    upper_end = old_ranks // 2
    offsets = jax.random.randint(key_new, (cells,), 0, 1 << 20, dtype=jnp.int32)
    new_ranks = lower_end + offsets % (upper_end - lower_end + 1)
    new_ranks = jnp.where(old_ranks == RMAX, upper_end, new_ranks)
    return (old_ranks.reshape(TILE_ROWS, TILE_COLS).astype(jnp.int32), new_ranks.reshape(TILE_ROWS, TILE_COLS).astype(jnp.int32))


def draw_row_rank(key, part):
    return panel_ranks(key, 13, TILE_ROWS)


def draw_col_rank(key, part):
    return panel_ranks(key, 29, TILE_COLS)


def draw_old_rank(key, part):
    return rank_pair(key)[0]


def draw_new_rank(key, part):
    return rank_pair(key)[1]


def draw_diag_inverse(key, part):
    key_off, key_diag = jax.random.split(jax.random.fold_in(key, 17))
    spread = 0.5 / jnp.sqrt(jnp.float32(NB))
    raw = jnp.clip(jax.random.normal(key_off, (NB, NB), jnp.float32), -3.5, 3.5) * spread
    diagonal = jax.random.uniform(key_diag, (NB,), jnp.float32, 0.3, 0.45)
    lower = jnp.tril(raw, -1)
    return (lower + jnp.diag(diagonal)).astype(jnp.bfloat16)


def level_of(own_key, dims, cuts, low, top_value):
    def one(axis_at, parts):
        draws = jax.random.uniform(jax.random.fold_in(jax.random.fold_in(own_key, 6), axis_at), (parts,), jnp.float32, low / len(cuts), top_value / len(cuts))
        return jnp.repeat(jnp.exp(draws), dims[axis_at] // parts).reshape((-1,) + (1,) * (len(dims) - axis_at - 1))

    factor_of = one(*cuts[0])
    for cut in cuts[1:]:
        factor_of = factor_of * one(*cut)
    return factor_of


def scatter_about(key, extent, width, limit, cuts=(), kind=jnp.bfloat16):
    level = level_of(key, extent, cuts, -0.22, 0.18) if cuts else 1.0
    values = jax.random.normal(key, extent, jnp.float32) * width * level
    return jnp.minimum(jnp.maximum(values, -limit), limit).astype(kind)


def setup_inputs(seed: int = 0) -> dict:
    splits = jax.random.split(jax.random.key(seed), 13)
    return {
        "diag_inverse": draw_diag_inverse(jax.random.fold_in(splits[12], 71), 0),
        "row_u": scatter_about(splits[1], (TILE_ROWS, NB, RMAX), 1.0, 6.0, ((0, 4), (2, 8))),
        "row_v": scatter_about(splits[2], (TILE_ROWS, NB, RMAX), 0.1, 0.59765625, ((0, 4), (2, 8))),
        "col_u": scatter_about(splits[3], (TILE_COLS, NB, RMAX), 1.0, 6.0, ((0, 8), (2, 4))),
        "col_v": scatter_about(splits[4], (TILE_COLS, NB, RMAX), 0.1, 0.59765625, ((0, 8), (2, 4))),
        "tile_u": scatter_about(splits[5], (TILE_ROWS, TILE_COLS, NB, RMAX), 1.0, 6.0, ((0, 4), (1, 8))),
        "tile_v": scatter_about(splits[6], (TILE_ROWS, TILE_COLS, NB, RMAX), 1.0, 6.0, ((0, 4), (1, 8))),
        "sketch": scatter_about(splits[7], (NB, RMAX), 1.0, 6.0),
        "row_rank": draw_row_rank(jax.random.fold_in(splits[12], 71), 0),
        "col_rank": draw_col_rank(jax.random.fold_in(splits[12], 71), 0),
        "old_rank": draw_old_rank(jax.random.fold_in(splits[12], 71), 0),
        "new_rank": draw_new_rank(jax.random.fold_in(splits[12], 71), 0),
    }


precise_mode = lax.Precision.HIGHEST

def keep_mask(rank_cap, count):
    return jnp.arange(rank_cap, dtype=jnp.int32) < count

def solve_panel(inverse, right_side, counts):
    tile_count, row_count, rank_cap = right_side.shape
    keep_cols = jnp.arange(rank_cap, dtype=jnp.int32)[None, None, :] < counts[:, None, None]
    values = jnp.where(keep_cols, right_side, jnp.zeros_like(right_side))
    stacked = jnp.transpose(values, (1, 0, 2)).reshape(row_count, tile_count * rank_cap)
    solved = jnp.dot(inverse.astype(jnp.float32), stacked.astype(jnp.float32), preferred_element_type=jnp.float32)
    return jnp.transpose(solved.reshape(row_count, tile_count, rank_cap), (1, 0, 2)).astype(jnp.bfloat16)

def tile_update(base_u, base_v, left_u, left_w, right_u, right_w, sketch, old_count, new_count):
    row_count, rank_cap = base_u.shape
    kept_v = jnp.where(keep_mask(rank_cap, old_count)[None, :], base_v, jnp.zeros_like(base_v))
    new_keep = keep_mask(rank_cap, new_count)
    probe_cols = jnp.where(new_keep[None, :], sketch, jnp.zeros_like(sketch))
    core_mat = jnp.dot(left_w.T.astype(jnp.float32), right_w.astype(jnp.float32), preferred_element_type=jnp.float32).astype(jnp.bfloat16)
    left_small = jnp.dot(kept_v.T.astype(jnp.float32), probe_cols.astype(jnp.float32), preferred_element_type=jnp.float32).astype(jnp.bfloat16)
    across = jnp.dot(right_u.T.astype(jnp.float32), probe_cols.astype(jnp.float32), preferred_element_type=jnp.float32).astype(jnp.bfloat16)
    middle = jnp.dot(core_mat.astype(jnp.float32), across.astype(jnp.float32), preferred_element_type=jnp.float32).astype(jnp.bfloat16)
    range_y = jnp.dot(base_u.astype(jnp.float32), left_small.astype(jnp.float32), preferred_element_type=jnp.float32) - jnp.dot(left_u.astype(jnp.float32), middle.astype(jnp.float32), preferred_element_type=jnp.float32)
    padding = jnp.where(new_keep, 0.0, 1.0).astype(jnp.float32)
    gram = jnp.dot(range_y.T.astype(jnp.float32), range_y.astype(jnp.float32), precision=precise_mode, preferred_element_type=jnp.float32) + jnp.diag(padding)
    gram_factor = jnp.linalg.cholesky(gram)
    range_basis = jax.scipy.linalg.solve_triangular(gram_factor, range_y.T, lower=True).T
    new_u = (jnp.sqrt(jnp.float32(row_count)) * range_basis).astype(jnp.bfloat16)
    back_small = jnp.dot(base_u.T.astype(jnp.float32), new_u.astype(jnp.float32), preferred_element_type=jnp.float32).astype(jnp.bfloat16)
    side_small = jnp.dot(left_u.T.astype(jnp.float32), new_u.astype(jnp.float32), preferred_element_type=jnp.float32).astype(jnp.bfloat16)
    turned = jnp.dot(core_mat.T.astype(jnp.float32), side_small.astype(jnp.float32), preferred_element_type=jnp.float32).astype(jnp.bfloat16)
    summed = jnp.dot(kept_v.astype(jnp.float32), back_small.astype(jnp.float32), preferred_element_type=jnp.float32) - jnp.dot(right_u.astype(jnp.float32), turned.astype(jnp.float32), preferred_element_type=jnp.float32)
    new_v = (summed / jnp.float32(row_count)).astype(jnp.bfloat16)
    return (new_u, new_v)

def reference(diag_inverse, row_u, row_v, col_u, col_v, tile_u, tile_v, sketch, row_rank, col_rank, old_rank, new_rank):
    row_solved = solve_panel(diag_inverse, row_v, row_rank)
    col_solved = solve_panel(diag_inverse, col_v, col_rank)
    col_indices = jnp.arange(TILE_COLS, dtype=jnp.int32)

    def one_row(row_index):

        def one_tile(col_index):
            return tile_update(tile_u[row_index, col_index], tile_v[row_index, col_index], row_u[row_index], row_solved[row_index], col_u[col_index], col_solved[col_index], sketch, old_rank[row_index, col_index], new_rank[row_index, col_index])
        return lax.map(one_tile, col_indices)
    new_u, new_v = lax.map(one_row, jnp.arange(TILE_ROWS, dtype=jnp.int32))
    return (new_u, new_v)
```

```python
import functools

import jax
import jax.numpy as jnp
from jax import lax
from jax.experimental import pallas as pl
from jax.experimental.pallas import tpu as pltpu
from jax.sharding import PartitionSpec as P

FULL = lax.Precision.HIGHEST
NT = (((1,), (1,)), ((), ()))
NN = (((1,), (0,)), ((), ()))
LANES = 128
SUBLANES = 8
PACK = 16


def dot_nt(a, b, precision=None):
    return lax.dot_general(a, b, NT, precision=precision, preferred_element_type=jnp.float32)


def dot_nn(a, b, precision=None):
    return lax.dot_general(a, b, NN, precision=precision, preferred_element_type=jnp.float32)


def round_up(n, m):
    return (n + m - 1) // m * m


def by_pairs(n):
    return n <= 8 and n & (n - 1) == 0


def swap(x, axis, n, k):
    return lax.ppermute(x, axis, [(i, i ^ k) for i in range(n)])


def spread(x, axis, n):
    if n == 1:
        return [x]
    if by_pairs(n):
        return [x] + [swap(x, axis, n, k) for k in range(1, n)]
    every = lax.all_gather(x, axis)
    return [every[k] for k in range(n)]


def spread_near(x, axis, n):
    if n < 4 or not by_pairs(n):
        return spread(x, axis, n)
    even = [x] + [swap(x, axis, n, k) for k in range(2, n, 2)]
    odd = [swap(e, axis, n, 1) for e in even]
    return [(odd if k % 2 else even)[k // 2] for k in range(n)]


def hand_out(parts, axis, n):
    if n == 1:
        return parts
    if by_pairs(n):
        return [parts[0]] + [swap(parts[k], axis, n, k) for k in range(1, n)]
    got = lax.all_to_all(jnp.stack(parts), axis, 0, 0)
    return [got[k] for k in range(n)]


def source_of(own, k, n):
    return own ^ k if by_pairs(n) else k


def call(body, out_shape, n_smem, n_vmem, scratch=()):
    return pl.pallas_call(
        body,
        out_shape=out_shape,
        in_specs=[pl.BlockSpec(memory_space=pltpu.SMEM)] * n_smem
        + [pl.BlockSpec(memory_space=pltpu.VMEM)] * n_vmem,
        scratch_shapes=list(scratch),
        compiler_params=pltpu.CompilerParams(vmem_limit_bytes=56 * 1024 * 1024),
    )


def row_solve_body(*refs, pad):
    *chunks, inverse, out, stacked = refs
    stacked[...] = jnp.zeros_like(stacked)
    width = chunks[0].shape[0]
    for k, chunk in enumerate(chunks):
        stacked[k * pad : k * pad + width, :] = chunk[...]
    out[...] = dot_nt(stacked[...], inverse[...]).astype(jnp.bfloat16)


def core_body(*refs, n_row, n_col, row_pad, col_pad):
    own, refs = refs[0], refs[1:]
    col_chunks, refs = refs[:n_row], refs[n_row:]
    inverse, refs = refs[0], refs[1:]
    solved, refs = refs[:n_col], refs[n_col:]
    outs, stacked = refs[:n_row], refs[n_row]
    stacked[...] = jnp.zeros_like(stacked)
    width = col_chunks[0].shape[0]
    for k, chunk in enumerate(col_chunks):
        at = source_of(own[0], k, n_row)
        stacked[pl.ds(pl.multiple_of(at * col_pad, col_pad), width), :] = chunk[...]
    col_solved = dot_nt(stacked[...], inverse[...]).astype(jnp.bfloat16)
    for m in range(n_col):
        part = dot_nt(solved[m][...], col_solved).astype(jnp.bfloat16)
        for k in range(n_row):
            outs[k][m * row_pad : (m + 1) * row_pad, :] = part[k * row_pad : (k + 1) * row_pad, :]


def lane_spread(x, lane):
    return jnp.broadcast_to(x[:, lane : lane + 1], x.shape)


def row_spread(x, row):
    return jnp.broadcast_to(x[row : row + 1, :], x.shape)


def inverse_factor(gram, live):
    size = gram.shape[0]
    blocks = size // SUBLANES
    live_blocks = live // SUBLANES if live % SUBLANES == 0 else blocks
    sub = lax.broadcasted_iota(jnp.int32, (SUBLANES, size), 0)
    lane = lax.broadcasted_iota(jnp.int32, (SUBLANES, size), 1)
    left = [gram[i * SUBLANES : (i + 1) * SUBLANES, :] for i in range(blocks)]
    right = [jnp.where(lane == sub + i * SUBLANES, 1.0, 0.0).astype(jnp.float32) for i in range(blocks)]
    for b in range(live_blocks):
        cols = {
            (i, q): lane_spread(left[i], b * SUBLANES + q)
            for i in range(b, live_blocks)
            for q in range(SUBLANES)
        }
        scale = jnp.zeros((SUBLANES, size), jnp.float32)
        for q in range(SUBLANES):
            root = lax.rsqrt(row_spread(cols[b, q], q))
            scale = jnp.where(sub == q, root, scale)
            square = root * root
            left_row = row_spread(left[b], q)
            right_row = row_spread(right[b], q)
            heads = {p: row_spread(cols[b, p], q) for p in range(q + 1, SUBLANES)}
            for i in range(b, live_blocks):
                times = cols[i, q] * square
                if i == b:
                    times = jnp.where(sub > q, times, 0.0)
                left[i] = left[i] - times * left_row
                right[i] = right[i] - times * right_row
                for p in range(q + 1, SUBLANES):
                    cols[i, p] = cols[i, p] - times * heads[p]
        right[b] = right[b] * scale
    return jnp.concatenate(right, axis=0)


def tile_body(*refs, n_row, n_col, row_pad, col_pad, half):
    (own_col, own_row, row_rank, col_rank, old_rank, new_rank), refs = refs[:6], refs[6:]
    cores, refs = refs[:n_row], refs[n_row:]
    row_chunks, refs = refs[:n_col], refs[n_col:]
    col_chunks, refs = refs[:n_row], refs[n_row:]
    base_u, base_v, sketch, new_u, new_v, left_u, right_u = refs
    rank_cap, row_count = base_u.shape
    row_width, col_width = row_chunks[0].shape[0], col_chunks[0].shape[0]
    n_p, n_q = n_col * row_pad, n_row * col_pad

    left_u[...] = jnp.zeros_like(left_u)
    for m, chunk in enumerate(row_chunks):
        left_u[m * row_pad : m * row_pad + row_width, :] = chunk[...]
    right_u[...] = jnp.zeros_like(right_u)
    for k, chunk in enumerate(col_chunks):
        at = source_of(own_row[0], k, n_row)
        right_u[pl.ds(pl.multiple_of(at * col_pad, col_pad), col_width), :] = chunk[...]

    total = cores[0][...].astype(jnp.float32)
    for k in range(1, n_row):
        total = total + cores[k][...].astype(jnp.float32)
    p_at = lax.broadcasted_iota(jnp.int32, (n_p, n_q), 0)
    q_at = lax.broadcasted_iota(jnp.int32, (n_p, n_q), 1)
    q_at = lax.div(q_at, col_pad) * col_width + lax.rem(q_at, col_pad)
    p_chunk, p_in = lax.div(p_at, row_pad), lax.rem(p_at, row_pad)
    p_source = lax.bitwise_xor(p_chunk, own_col[0]) if by_pairs(n_col) else p_chunk
    p_at = p_source * row_width + p_in
    keep = (p_at < row_rank[0]) & (q_at < col_rank[0])
    core = jnp.where(keep, total, 0.0).astype(jnp.bfloat16)

    old_at = lax.broadcasted_iota(jnp.int32, (rank_cap, row_count), 0)
    kept_v = jnp.where(old_at < old_rank[0, 0], base_v[...], jnp.zeros_like(base_v))
    new_at = lax.broadcasted_iota(jnp.int32, (half, row_count), 0)
    probe = sketch[0:half, :]
    probe = jnp.where(new_at < new_rank[0, 0], probe, jnp.zeros_like(probe))

    left_small = dot_nt(probe, kept_v).astype(jnp.bfloat16)
    across = dot_nt(probe, right_u[...]).astype(jnp.bfloat16)
    middle = dot_nt(across, core).astype(jnp.bfloat16)
    range_y = dot_nn(left_small, base_u[...]) - dot_nn(middle, left_u[...])
    diag_at = lax.broadcasted_iota(jnp.int32, (half, half), 0)
    diag_on = diag_at == lax.broadcasted_iota(jnp.int32, (half, half), 1)
    padding = jnp.where(diag_on & (diag_at >= new_rank[0, 0]), 1.0, 0.0)
    gram = dot_nt(range_y, range_y, FULL) + padding
    basis = dot_nn(inverse_factor(gram, min(half, round_up(rank_cap // 2, SUBLANES))), range_y, FULL)
    out_u = (jnp.sqrt(jnp.float32(row_count)) * basis).astype(jnp.bfloat16)
    back_small = dot_nt(out_u, base_u[...]).astype(jnp.bfloat16)
    side_small = dot_nt(out_u, left_u[...]).astype(jnp.bfloat16)
    turned = dot_nn(side_small, core).astype(jnp.bfloat16)
    summed = dot_nn(back_small, kept_v) - dot_nn(turned, right_u[...])
    new_u[0:half, :] = out_u
    new_v[0:half, :] = (summed / jnp.float32(row_count)).astype(jnp.bfloat16)
    if half < rank_cap:
        new_u[half:, :] = jnp.zeros((rank_cap - half, row_count), jnp.bfloat16)
        new_v[half:, :] = jnp.zeros((rank_cap - half, row_count), jnp.bfloat16)


def on_device(
    diag_inverse,
    row_u,
    row_v,
    col_u,
    col_v,
    tile_u,
    tile_v,
    sketch,
    row_rank,
    col_rank,
    old_rank,
    new_rank,
    n_row,
    n_col,
):
    own_row = jnp.reshape(lax.axis_index("row").astype(jnp.int32), (1,))
    own_col = jnp.reshape(lax.axis_index("col").astype(jnp.int32), (1,))
    row_share, row_count = diag_inverse.shape
    rank_cap = tile_u.shape[3]
    row_width, col_width = row_v.shape[2], col_v.shape[2]
    row_pad, col_pad = round_up(row_width, PACK), round_up(col_width, PACK)
    n_p, n_q = n_col * row_pad, n_row * col_pad
    half = min(round_up(rank_cap // 2, LANES), rank_cap)
    bf16 = jnp.bfloat16
    shape = jax.ShapeDtypeStruct

    row_chunks = spread(row_v[0].T, "row", n_row)
    col_chunks = spread(col_v[0].T, "row", n_row)
    right_chunks = spread(col_u[0].T, "row", n_row)
    solved = call(
        functools.partial(row_solve_body, pad=row_pad),
        shape((n_row * row_pad, row_share), bf16),
        0,
        n_row + 1,
        [pltpu.VMEM((n_row * row_pad, row_count), bf16)],
    )(*row_chunks, diag_inverse)
    solved = spread_near(solved, "col", n_col)
    left_chunks = spread_near(row_u[0].T, "col", n_col)
    parts = call(
        functools.partial(core_body, n_row=n_row, n_col=n_col, row_pad=row_pad, col_pad=col_pad),
        [shape((n_p, n_q), bf16)] * n_row,
        1,
        n_row + 1 + n_col,
        [pltpu.VMEM((n_q, row_count), bf16)],
    )(own_row, *col_chunks, diag_inverse, *solved)
    cores = hand_out(list(parts), "row", n_row)
    new_u, new_v = call(
        functools.partial(
            tile_body, n_row=n_row, n_col=n_col, row_pad=row_pad, col_pad=col_pad, half=half
        ),
        [shape((rank_cap, row_count), bf16)] * 2,
        6,
        2 * n_row + n_col + 3,
        [pltpu.VMEM((n_p, row_count), bf16), pltpu.VMEM((n_q, row_count), bf16)],
    )(
        own_col,
        own_row,
        row_rank,
        col_rank,
        old_rank,
        new_rank,
        *cores,
        *left_chunks,
        *right_chunks,
        tile_u[0, 0].T,
        tile_v[0, 0].T,
        sketch.T,
    )
    return (new_u.T[None, None], new_v.T[None, None])


def solution(mesh):
    in_specs = (
        P("row", None),
        P("row", None, "col"),
        P("row", None, "col"),
        P("col", None, "row"),
        P("col", None, "row"),
        P("row", "col", None, None),
        P("row", "col", None, None),
        P(),
        P("row"),
        P("col"),
        P("row", "col"),
        P("row", "col"),
    )
    out_specs = (P("row", "col", None, None), P("row", "col", None, None))
    body = functools.partial(on_device, n_row=mesh.shape["row"], n_col=mesh.shape["col"])
    return jax.shard_map(body, mesh=mesh, in_specs=in_specs, out_specs=out_specs, check_vma=False)
```

```python
import functools

import jax
import jax.numpy as jnp
from jax import lax
from jax.experimental import pallas as pl
from jax.experimental.pallas import tpu as pltpu
from jax.sharding import PartitionSpec as P


FULL = lax.Precision.HIGHEST
NT = (((1,), (1,)), ((), ()))
NN = (((1,), (0,)), ((), ()))
LANES = 128
SUBLANES = 8
PACK = 16


def dot_nt(a, b, precision=None):
    return lax.dot_general(a, b, NT, precision=precision, preferred_element_type=jnp.float32)


def dot_nn(a, b, precision=None):
    return lax.dot_general(a, b, NN, precision=precision, preferred_element_type=jnp.float32)


def round_up(n, m):
    return (n + m - 1) // m * m


def by_pairs(n):
    return n <= 8 and n & (n - 1) == 0


def swap(x, axis, n, k):
    return lax.ppermute(x, axis, [(i, i ^ k) for i in range(n)])


def spread(x, axis, n):
    if n == 1:
        return [x]
    if by_pairs(n):
        return [x] + [swap(x, axis, n, k) for k in range(1, n)]
    every = lax.all_gather(x, axis)
    return [every[k] for k in range(n)]


def spread_near(x, axis, n):
    if n < 4 or not by_pairs(n):
        return spread(x, axis, n)
    even = [x] + [swap(x, axis, n, k) for k in range(2, n, 2)]
    odd = [swap(e, axis, n, 1) for e in even]
    return [(odd if k % 2 else even)[k // 2] for k in range(n)]


def hand_out(parts, axis, n):
    if n == 1:
        return parts
    if by_pairs(n):
        return [parts[0]] + [swap(parts[k], axis, n, k) for k in range(1, n)]
    got = lax.all_to_all(jnp.stack(parts), axis, 0, 0)
    return [got[k] for k in range(n)]


def source_of(own, k, n):
    return own ^ k if by_pairs(n) else k


def call(body, out_shape, smem, vmem, scratch=(), small=True):
    outs = [jax.ShapeDtypeStruct(dims, dtype) for dims, dtype in out_shape]
    return pl.pallas_call(
        body,
        out_shape=outs,
        in_specs=[pl.BlockSpec(memory_space=pltpu.SMEM)] * len(smem)
        + [pl.BlockSpec(memory_space=pltpu.VMEM)] * len(vmem),
        out_specs=[pl.BlockSpec(memory_space=pltpu.VMEM)] * len(outs),
        scratch_shapes=list(scratch),
        compiler_params=pltpu.CompilerParams(vmem_limit_bytes=(12 if small else 56) * 2**20),
    )(*smem, *vmem)


def row_solve_body(*refs, pad):
    *chunks, inverse, out, stacked = refs
    stacked[...] = jnp.zeros_like(stacked)
    width = chunks[0].shape[0]
    for k, chunk in enumerate(chunks):
        stacked[k * pad : k * pad + width, :] = chunk[...]
    out[...] = dot_nt(stacked[...], inverse[...]).astype(jnp.bfloat16)


def core_body(*refs, n_row, n_col, row_pad, col_pad):
    own_row = lax.axis_index("row")
    col_chunks, refs = refs[:n_row], refs[n_row:]
    inverse, refs = refs[0], refs[1:]
    solved, refs = refs[:n_col], refs[n_col:]
    outs, stacked = refs[:n_row], refs[n_row]
    stacked[...] = jnp.zeros_like(stacked)
    width = col_chunks[0].shape[0] // 2
    for k, chunk in enumerate(col_chunks):
        at = source_of(own_row, k, n_row)
        stacked[pl.ds(pl.multiple_of(at * col_pad, col_pad), width), :] = chunk[0:width, :]
    col_solved = dot_nt(stacked[...], inverse[...]).astype(jnp.bfloat16)
    for m in range(n_col):
        part = dot_nt(solved[m][...], col_solved).astype(jnp.bfloat16)
        for k in range(n_row):
            outs[k][m * row_pad : (m + 1) * row_pad, :] = part[k * row_pad : (k + 1) * row_pad, :]


def lane_spread(x, lane):
    return jnp.broadcast_to(x[:, lane : lane + 1], x.shape)


def row_spread(x, row):
    return jnp.broadcast_to(x[row : row + 1, :], x.shape)


def inverse_factor(gram, live):
    size = gram.shape[0]
    blocks = size // SUBLANES
    live_blocks = live // SUBLANES if live % SUBLANES == 0 else blocks
    sub = lax.broadcasted_iota(jnp.int32, (SUBLANES, size), 0)
    lane = lax.broadcasted_iota(jnp.int32, (SUBLANES, size), 1)
    left = [gram[i * SUBLANES : (i + 1) * SUBLANES, :] for i in range(blocks)]
    right = [jnp.where(lane == sub + i * SUBLANES, 1.0, 0.0).astype(jnp.float32) for i in range(blocks)]
    for b in range(live_blocks):
        cols = {
            (i, q): lane_spread(left[i], b * SUBLANES + q)
            for i in range(b, live_blocks)
            for q in range(SUBLANES)
        }
        scale = jnp.zeros((SUBLANES, size), jnp.float32)
        for q in range(SUBLANES):
            root = lax.rsqrt(row_spread(cols[b, q], q))
            scale = jnp.where(sub == q, root, scale)
            square = root * root
            left_row = row_spread(left[b], q)
            right_row = row_spread(right[b], q)
            heads = {p: row_spread(cols[b, p], q) for p in range(q + 1, SUBLANES)}
            for i in range(b, live_blocks):
                times = cols[i, q] * square
                if i == b:
                    times = jnp.where(sub > q, times, 0.0)
                left[i] = left[i] - times * left_row
                right[i] = right[i] - times * right_row
                for p in range(q + 1, SUBLANES):
                    cols[i, p] = cols[i, p] - times * heads[p]
        right[b] = right[b] * scale
    return jnp.concatenate(right, axis=0)


def base_body(*refs, n_row, col_pad, half):
    old_rank, new_rank, *refs = refs
    own_row = lax.axis_index("row")
    col_chunks, refs = refs[:n_row], refs[n_row:]
    base_u, base_v, sketch, right_u, across, base_y = refs
    rank_cap, row_count = base_u.shape
    width = col_chunks[0].shape[0] // 2
    right_u[...] = jnp.zeros_like(right_u)
    for k, chunk in enumerate(col_chunks):
        at = source_of(own_row, k, n_row)
        right_u[pl.ds(pl.multiple_of(at * col_pad, col_pad), width), :] = chunk[width : 2 * width, :]
    old_at = lax.broadcasted_iota(jnp.int32, (rank_cap, row_count), 0)
    kept_v = jnp.where(old_at < old_rank[0, 0], base_v[...], jnp.zeros_like(base_v))
    new_at = lax.broadcasted_iota(jnp.int32, (half, row_count), 0)
    probe = sketch[0:half, :]
    probe = jnp.where(new_at < new_rank[0, 0], probe, jnp.zeros_like(probe))
    left_small = dot_nt(probe, kept_v).astype(jnp.bfloat16)
    across[...] = dot_nt(probe, right_u[...]).astype(jnp.bfloat16)
    base_y[...] = dot_nn(left_small, base_u[...])


def tile_body(*refs, n_row, n_col, row_pad, col_pad, row_width, col_width, half):
    (row_rank, col_rank, old_rank, new_rank), refs = refs[:4], refs[4:]
    own_col = lax.axis_index("col")
    cores, refs = refs[:n_row], refs[n_row:]
    row_chunks, refs = refs[:n_col], refs[n_col:]
    right_u, across, base_y, base_u, base_v, new_u, new_v, left_u = refs
    rank_cap, row_count = base_u.shape
    n_p, n_q = n_col * row_pad, n_row * col_pad

    left_u[...] = jnp.zeros_like(left_u)
    for m, chunk in enumerate(row_chunks):
        left_u[m * row_pad : m * row_pad + row_width, :] = chunk[...]
    total = cores[0][...].astype(jnp.float32)
    for k in range(1, n_row):
        total = total + cores[k][...].astype(jnp.float32)
    p_at = lax.broadcasted_iota(jnp.int32, (n_p, n_q), 0)
    q_at = lax.broadcasted_iota(jnp.int32, (n_p, n_q), 1)
    q_at = lax.div(q_at, col_pad) * col_width + lax.rem(q_at, col_pad)
    p_chunk, p_in = lax.div(p_at, row_pad), lax.rem(p_at, row_pad)
    p_source = lax.bitwise_xor(p_chunk, own_col) if by_pairs(n_col) else p_chunk
    p_at = p_source * row_width + p_in
    keep = (p_at < row_rank[0]) & (q_at < col_rank[0])
    core = jnp.where(keep, total, 0.0).astype(jnp.bfloat16)

    middle = dot_nt(across[...], core).astype(jnp.bfloat16)
    range_y = base_y[...] - dot_nn(middle, left_u[...])
    diag_at = lax.broadcasted_iota(jnp.int32, (half, half), 0)
    diag_on = diag_at == lax.broadcasted_iota(jnp.int32, (half, half), 1)
    padding = jnp.where(diag_on & (diag_at >= new_rank[0, 0]), 1.0, 0.0)
    gram = dot_nt(range_y, range_y, FULL) + padding
    basis = dot_nn(inverse_factor(gram, min(half, round_up(rank_cap // 2, SUBLANES))), range_y, FULL)
    out_u = (jnp.sqrt(jnp.float32(row_count)) * basis).astype(jnp.bfloat16)
    back_small = dot_nt(out_u, base_u[...]).astype(jnp.bfloat16)
    side_small = dot_nt(out_u, left_u[...]).astype(jnp.bfloat16)
    turned = dot_nn(side_small, core).astype(jnp.bfloat16)
    old_at = lax.broadcasted_iota(jnp.int32, (half, rank_cap), 1)
    back_small = jnp.where(old_at < old_rank[0, 0], back_small, jnp.zeros_like(back_small))
    summed = dot_nn(back_small, base_v[...]) - dot_nn(turned, right_u[...])
    new_u[0:half, :] = out_u
    new_v[0:half, :] = (summed / jnp.float32(row_count)).astype(jnp.bfloat16)
    if half < rank_cap:
        new_u[half:, :] = jnp.zeros((rank_cap - half, row_count), jnp.bfloat16)
        new_v[half:, :] = jnp.zeros((rank_cap - half, row_count), jnp.bfloat16)


def on_device(
    diag_inverse,
    row_u,
    row_v,
    col_u,
    col_v,
    tile_u,
    tile_v,
    sketch,
    row_rank,
    col_rank,
    old_rank,
    new_rank,
    n_row,
    n_col,
):
    row_share, row_count = diag_inverse.shape
    rank_cap = tile_u.shape[3]
    row_width, col_width = row_v.shape[2], col_v.shape[2]
    row_pad, col_pad = round_up(row_width, PACK), round_up(col_width, PACK)
    n_p, n_q = n_col * row_pad, n_row * col_pad
    half = min(round_up(rank_cap // 2, LANES), rank_cap)
    bf16 = jnp.bfloat16
    sizes = dict(n_row=n_row, row_pad=row_pad, col_pad=col_pad, n_col=n_col)
    base_u, base_v = tile_u[0, 0].T, tile_v[0, 0].T
    small = by_pairs(n_row) and by_pairs(n_col)

    row_chunks = spread(row_v[0].T, "row", n_row)
    col_chunks = spread(jnp.concatenate([col_v[0].T, col_u[0].T], axis=0), "row", n_row)
    (solved,) = call(
        functools.partial(row_solve_body, pad=row_pad),
        [((n_row * row_pad, row_share), bf16)],
        [],
        [*row_chunks, diag_inverse],
        [pltpu.VMEM((n_row * row_pad, row_count), bf16)],
        small=small,
    )
    solved = spread_near(solved, "col", n_col)
    left_chunks = spread_near(row_u[0].T, "col", n_col)
    parts = call(
        functools.partial(core_body, **sizes),
        [((n_p, n_q), bf16)] * n_row,
        [],
        [*col_chunks, diag_inverse, *solved],
        [pltpu.VMEM((n_q, row_count), bf16)],
        small=small,
    )
    cores = hand_out(list(parts), "row", n_row)
    right_u, across, base_y = call(
        functools.partial(base_body, n_row=n_row, col_pad=col_pad, half=half),
        [((n_q, row_count), bf16), ((half, n_q), bf16), ((half, row_count), jnp.float32)],
        [old_rank, new_rank],
        [*col_chunks, base_u, base_v, sketch.T],
        small=small,
    )
    new_u, new_v = call(
        functools.partial(
            tile_body, **sizes, row_width=row_width, col_width=col_width, half=half
        ),
        [((rank_cap, row_count), bf16)] * 2,
        [row_rank, col_rank, old_rank, new_rank],
        [*cores, *left_chunks, right_u, across, base_y, base_u, base_v],
        [pltpu.VMEM((n_p, row_count), bf16)],
        small=small,
    )
    return (new_u.T[None, None], new_v.T[None, None])


def solution(mesh):
    in_specs = (
        P("row", None),
        P("row", None, "col"),
        P("row", None, "col"),
        P("col", None, "row"),
        P("col", None, "row"),
        P("row", "col", None, None),
        P("row", "col", None, None),
        P(),
        P("row"),
        P("col"),
        P("row", "col"),
        P("row", "col"),
    )
    out_specs = (P("row", "col", None, None), P("row", "col", None, None))
    body = functools.partial(on_device, n_row=mesh.shape["row"], n_col=mesh.shape["col"])

    return jax.shard_map(body, mesh=mesh, in_specs=in_specs, out_specs=out_specs, check_vma=False)
```
